32 devices in a mesh: tp: 4 (over z), pp: 8 (over y, x, core).
Axes of the slice: x: 2, y: 2, z: 4, core: 2. Of those that a mesh axis runs over, the one named last changes fastest.
Arguments:
- tokens: bfloat16 [8192, 8192], P('pp', 'tp'), may hold values from -60 to 60
- norm_gain: bfloat16 [8192], P('tp'), may hold values from 0.099609375 to 1.8984375
- weights_gen: bfloat16 [8, 1280, 8192], P('tp', None, 'pp'), may hold values from -2 to 2
- segment_ids: int32 [8, 1024], P('pp'), may hold values from 0 to 15, never falling along the last dimension, each value on 1 to 512 neighbouring positions
Outputs:
- weights_rows: bfloat16 [8, 1280, 8192], P('tp', 'pp')
- attended: bfloat16 [8192, 8192], P('pp', 'tp')
The draws below stay inside these ranges and needn't reach their ends.
Inputs may be any that keep to these rules, and one draw needn't show every extreme that they name: `segment_ids`: ids never fall along a block; every sequence has 1 to 512 tokens and lies in one block.
All inputs are finite; a program needn't handle non-finite values.
Results may differ from the reference program's by a relative error of at most 0.0075.
Values may be sent and summed in bfloat16 or wider, within the bound.
A program may use at most 192 MiB of HBM per device.

```python
import math
import jax
import jax.numpy as jnp
import numpy as np
from jax import lax

D = 8192
HQ = 64
KVH = 8
DH = 128
TOK_DEV = 1024
GROUP = 8
QROWS = 1280
BLOCKS = 8
TOKENS = 8192
SEGS = 16


def draw_tokens(key, part):
    first = jax.random.fold_in(jax.random.fold_in(key, 11), 0)
    base = jax.random.truncated_normal(first, -6.0, 6.0, (TOKENS, D), jnp.float32)
    return jnp.clip(base, -60.0, 60.0).astype(jnp.bfloat16)


def draw_weights_gen(key, part):
    first = jax.random.fold_in(jax.random.fold_in(key, 23), 0)
    base = jax.random.truncated_normal(first, -6.0, 6.0, (KVH, QROWS, D), jnp.float32) / math.sqrt(D)
    return jnp.clip(base, -2.0, 2.0).astype(jnp.bfloat16)


def length_profile(count, total, limit, lean):
    portions = [(1 << 20) // math.isqrt(rank ** lean) + 1 for rank in range(2, count + 1)]
    rest, counts = total - limit - (count - 1), [1] * (count - 1)
    while rest > 0:
        candidates = [i for i in range(count - 1) if counts[i] < limit]
        whole, budget = sum([portions[i] for i in candidates]), rest
        for i in candidates:
            addition = min(limit - counts[i], max(1, budget * portions[i] // whole), rest)
            counts[i] = counts[i] + addition
            rest = rest - addition
    return np.array([limit] + counts)


def uneven_parts(rng, amount, total, limit, lean):
    if amount == 2:
        one = jax.random.randint(rng, (), max(1, total - limit), min(limit, total - 1) + 1)
        return jnp.stack([one, total - one])
    lengths = jnp.asarray(length_profile(amount, total, limit, lean), jnp.int32)
    pairs = (amount - 1) // 2
    donor, taker = lengths[1:1 + 2 * pairs:2], lengths[2:2 + 2 * pairs:2]
    margin = jnp.minimum(donor - 1, limit - taker)
    passed = jax.random.randint(jax.random.fold_in(rng, 1), (pairs,), 0, 1 << 20) % (margin + 1)
    lengths = lengths.at[1:1 + 2 * pairs:2].set(donor - passed).at[2:2 + 2 * pairs:2].set(taker + passed)
    return lengths[jax.random.permutation(jax.random.fold_in(rng, 2), amount)]


def setup_inputs(seed: int = 0) -> dict:
    splits = jax.random.split(jax.random.key(seed), 5)
    return {
        "tokens": draw_tokens(jax.random.fold_in(splits[4], 71), 0),
        "norm_gain": jnp.clip(1.0 + 0.18 * jax.random.normal(splits[1], (D,), jnp.float32), 0.099609375, 1.8984375).astype(jnp.bfloat16),
        "weights_gen": draw_weights_gen(jax.random.fold_in(splits[4], 71), 0),
        "segment_ids": jax.vmap(lambda own: jnp.searchsorted(jnp.cumsum(uneven_parts(own, SEGS, TOK_DEV, TOK_DEV // 2, 1)), jnp.arange(TOK_DEV), side="right"))(jax.random.split(splits[3], BLOCKS)).reshape((BLOCKS, TOK_DEV)).astype(jnp.int32),
    }


rope_base = 500000.0

def rotary(values, positions):
    half = values.shape[-1] // 2
    freq = jnp.exp(jnp.arange(half, dtype=jnp.float32) * (-2.0 * math.log(rope_base) / values.shape[-1]))
    angle = positions.astype(jnp.float32)[:, None] * freq[None, :]
    cosine = jnp.cos(angle)
    sine = jnp.sin(angle)
    extra = values.ndim - 2
    cosine = cosine.reshape(cosine.shape[:1] + (1,) * extra + cosine.shape[1:])
    sine = sine.reshape(sine.shape[:1] + (1,) * extra + sine.shape[1:])
    first = values[..., :half]
    second = values[..., half:]
    return jnp.concatenate([first * cosine - second * sine, second * cosine + first * sine], axis=-1)

def block_positions(seg):
    count = seg.shape[0]
    start = lax.optimization_barrier(jnp.sum((seg[None, :] < seg[:, None]).astype(jnp.int32), axis=1))
    return jnp.arange(count, dtype=jnp.int32) - start

def attend_block(query, key, value, seg):
    count = seg.shape[0]
    score = jnp.einsum('tgjd,sgd->gjts', query.astype(jnp.float32), key.astype(jnp.float32)) * (1.0 / math.sqrt(DH))
    order = jnp.arange(count, dtype=jnp.int32)
    allowed = (seg[:, None] == seg[None, :]) & (order[:, None] >= order[None, :])
    score = jnp.where(allowed[None, None], score, -1e+30)
    top = lax.optimization_barrier(jnp.max(score, axis=-1, keepdims=True))
    expo = jnp.where(allowed[None, None], jnp.exp(score - top), 0.0)
    prob = (expo / lax.optimization_barrier(jnp.sum(expo, axis=-1, keepdims=True))).astype(jnp.bfloat16)
    out = jnp.einsum('gjts,sgd->tgjd', prob.astype(jnp.float32), value.astype(jnp.float32))
    return out.astype(jnp.bfloat16).reshape(count, -1)

def reference(tokens, norm_gain, weights_gen, segment_ids):
    floats = tokens.astype(jnp.float32)
    square = lax.optimization_barrier(jnp.mean(floats * floats, axis=-1, keepdims=True))
    normed = (floats * lax.rsqrt(square + 1e-05) * norm_gain.astype(jnp.float32)).astype(jnp.bfloat16)
    flat = weights_gen.reshape(KVH * QROWS, D)
    mixed = jnp.dot(normed, flat.T, preferred_element_type=jnp.float32)
    mixed = mixed.reshape(TOKENS, KVH, GROUP + 2, DH)
    positions = jax.vmap(block_positions)(segment_ids).reshape(TOKENS)
    query = rotary(mixed[:, :, :GROUP, :], positions).astype(jnp.bfloat16)
    key = rotary(mixed[:, :, GROUP, :], positions).astype(jnp.bfloat16)
    value = mixed[:, :, GROUP + 1, :].astype(jnp.bfloat16)
    query = query.reshape(BLOCKS, TOK_DEV, KVH, GROUP, DH)
    key = key.reshape(BLOCKS, TOK_DEV, KVH, DH)
    value = value.reshape(BLOCKS, TOK_DEV, KVH, DH)

    def one_block(items):
        return attend_block(items[0], items[1], items[2], items[3])
    attended = lax.map(one_block, (query, key, value, segment_ids))
    return (weights_gen, attended.reshape(TOKENS, HQ * DH))
```

```python
import functools
import math

import jax
import jax.numpy as jnp
from jax import lax
from jax.experimental import pallas as pl
from jax.experimental.pallas import tpu as pltpu
from jax.sharding import PartitionSpec as P

DH = 128
GROUP = 8
HEADS = GROUP + 2
LANES = 128
MAX_SEQUENCE = 512
ROPE_BASE = 500000.0
EPS = 1e-05
PIECES = 4
MESH = pl.DeviceIdType.MESH
F32 = jnp.float32
BF16 = jnp.bfloat16


def project_kernel(
    n, pn, tokens, gain, seg, weights,
    wall, qkv,
    xr, xn, acc, wbuf, meta, rsb, ctab, stab, stage,
    own_sem, zs_sem, zr_sem, ms_sem, mr_sem, ws_sem, wr_sem, wf_sem, out_sem,
):
    me = lax.axis_index("tp")
    j = lax.axis_index("pp")
    count, local = tokens.shape
    rows, width = weights.shape
    half_rows = rows // 2
    per = local // width
    groups = qkv.shape[0]
    pr = count // PIECES
    rings = pn // 4
    blocks = count // LANES
    core, x, y = j % 2, (j // 2) % 2, j // 4

    def at(y_, x_, core_):
        return (y_ * 2 + x_) * 2 + core_

    j_x = at(y, 1 - x, core)
    j_next = at((y + 1) % rings, x, core)
    j_prev = at((y + rings - 1) % rings, x, core)
    j_pair = at(y, x, 1 - core)

    barrier = pltpu.get_barrier_semaphore()
    for d in range(1, n):
        pl.semaphore_signal(barrier, inc=1, device_id={"tp": (me + d) % n}, device_id_type=MESH)
    for other in (j_x, j_next, j_prev, j_pair):
        pl.semaphore_signal(barrier, inc=1, device_id={"pp": other}, device_id_type=MESH)
    pl.semaphore_wait(barrier, n - 1 + 4)

    def piece(slot, p, up, own=False):
        rng = pl.ds(p * pr, pr)
        return pltpu.make_async_remote_copy(
            src_ref=tokens.at[rng] if own else xr.at[slot, rng],
            dst_ref=xr.at[slot, rng],
            send_sem=zs_sem.at[1 if up else 0, slot, p],
            recv_sem=zr_sem.at[slot, p],
            device_id={"tp": me + 1 if up else me - 1},
            device_id_type=MESH,
        )

    def own_piece(p):
        @pl.when(me < n - 1)
        def _():
            piece(me, p, True, own=True).start()

        @pl.when(me > 0)
        def _():
            piece(me, p, False, own=True).start()

    started = []

    def send_half(link, shard, half, target, own=False):
        rng = pl.ds(half * half_rows, half_rows)
        copy = pltpu.make_async_remote_copy(
            src_ref=weights.at[rng] if own else wall.at[shard, rng],
            dst_ref=wall.at[shard, rng],
            send_sem=ws_sem.at[link, shard, half],
            recv_sem=wr_sem.at[shard, half],
            device_id={"pp": target},
            device_id_type=MESH,
        )
        copy.start()
        started.append(copy)

    def wait_half(shard, half):
        rng = pl.ds(half * half_rows, half_rows)
        pltpu.make_async_copy(wall.at[shard, rng], wall.at[shard, rng], wr_sem.at[shard, half]).wait()

    own_piece(0)
    send_half(0, j, 0, j_x, own=True)
    send_half(1, j, 1, j_next, own=True)
    send_half(0, j, 1, j_x, own=True)
    send_half(1, j, 0, j_next, own=True)
    send_half(2, j, 0, j_pair, own=True)
    send_half(2, j, 1, j_pair, own=True)

    load = pltpu.make_async_copy(tokens, xr.at[me], own_sem)
    load.start()
    load.wait()

    def squares(a, carry):
        v = xr[me, pl.ds(pl.multiple_of(a * LANES, LANES), LANES), :].astype(F32)
        total = jnp.sum(v * v, axis=1, keepdims=True)
        meta[me, pl.ds(a, 1), :] = jnp.broadcast_to(total, (LANES, LANES)).T[0:1, :]
        return carry

    lax.fori_loop(0, blocks, squares, 0)
    meta[me, blocks:, :] = gain[...]

    def meta_copy(d):
        return pltpu.make_async_remote_copy(
            src_ref=meta.at[me],
            dst_ref=meta.at[me],
            send_sem=ms_sem.at[d],
            recv_sem=mr_sem.at[me],
            device_id={"tp": (me + d) % n},
            device_id_type=MESH,
        )

    for d in range(1, n):
        meta_copy(d).start()
    for p in range(1, PIECES):
        own_piece(p)

    lane = lax.broadcasted_iota(jnp.int32, (LANES, LANES), 1)
    freq = jnp.exp((lane % (DH // 2)).astype(F32) * (-2.0 * math.log(ROPE_BASE) / DH))
    sign = jnp.where(lane < DH // 2, -1.0, 1.0)
    ids = seg[...].astype(F32)

    def tables(a, carry):
        rng = pl.ds(pl.multiple_of(a * LANES, LANES), LANES)
        own = jnp.broadcast_to(seg[:, rng].astype(F32), (LANES, LANES)).T[:, 0:1]
        first = jnp.sum(jnp.where(ids < own, 1.0, 0.0), axis=1, keepdims=True)
        order = (lax.broadcasted_iota(jnp.int32, (LANES, LANES), 0) + a * LANES).astype(F32)
        angle = (order - first) * freq
        ctab[rng, :] = jnp.cos(angle)
        stab[rng, :] = jnp.sin(angle) * sign
        return carry

    lax.fori_loop(0, blocks, tables, 0)

    def clear(a, carry):
        rng = pl.ds(pl.multiple_of(a * LANES, LANES), LANES)
        for half in range(2):
            acc[half, rng, :] = jnp.zeros((LANES, half_rows), F32)
        return carry

    lax.fori_loop(0, blocks, clear, 0)

    for d in range(1, n):
        other = (me + d) % n
        pltpu.make_async_copy(meta.at[other], meta.at[other], mr_sem.at[other]).wait()

    def scales(a, carry):
        total = meta[0, pl.ds(a, 1), :]
        for s in range(1, n):
            total = total + meta[s, pl.ds(a, 1), :]
        scale = lax.rsqrt(total * (1.0 / (n * local)) + EPS)
        rsb[pl.ds(pl.multiple_of(a * LANES, LANES), LANES), :] = jnp.broadcast_to(scale, (LANES, LANES)).T
        return carry

    lax.fori_loop(0, blocks, scales, 0)

    def normalise(slot, p):
        def block(a, carry):
            rng = pl.ds(pl.multiple_of(p * pr + a * LANES, LANES), LANES)
            scale = rsb[rng, :]
            for b in range(local // LANES):
                cols = slice(b * LANES, (b + 1) * LANES)
                v = xr[slot, rng, cols].astype(F32) * scale
                xn[slot, rng, cols] = (v * meta[slot, blocks + b : blocks + b + 1, :]).astype(BF16)
            return carry

        lax.fori_loop(0, pr // LANES, block, 0)

    near = jnp.minimum(me, n - 1 - me)

    def slot_of(o):
        pair = jnp.where(o % 2 == 1, me + (o + 1) // 2, me - (o + 1) // 2)
        return jnp.where(o <= 2 * near, pair, jnp.where(me <= n - 1 - me, o, n - 1 - o))

    def arrive(o, p):
        slot = slot_of(o)
        rng = pl.ds(p * pr, pr)
        pltpu.make_async_copy(xr.at[slot, rng], xr.at[slot, rng], zr_sem.at[slot, p]).wait()

        @pl.when((slot > me) & (me > 0))
        def _():
            piece(slot, p, False).start()

        @pl.when((slot < me) & (me < n - 1))
        def _():
            piece(slot, p, True).start()

    def each_piece(p, carry):
        normalise(me, p)
        return carry

    lax.fori_loop(0, PIECES, each_piece, 0)

    def events():
        result = []
        for s in range(1, rings):
            y_s = (y + rings - s) % rings
            on = s < rings - 1
            mine, across = at(y_s, x, core), at(y_s, 1 - x, core)
            result.append([(mine, 1, [(0, j_x)] + ([(1, j_next)] if on else []))])
            if s == 1:
                result[-1].append((j_x, 0, [(1, j_next)]))
            result.append([(mine, 0, [(1, j_next)] if on else [])])
            if s == 1:
                result[-1].append((j_x, 1, []))
            result.append([(across, 0, [(1, j_next)] if on else []), (across, 1, [])])
        return result

    pending = events()

    def take_weights():
        for shard, half, links in pending.pop(0):
            wait_half(shard, half)
            for link, target in links:
                send_half(link, shard, half, target)
            send_half(2, shard, half, j_pair)

    total = (n - 2) * PIECES
    step = max(1, total // len(pending))
    for o in range(1, n - 1):
        for p in range(PIECES):
            arrive(o, p)
            normalise(slot_of(o), p)
            done = (o - 1) * PIECES + p + 1
            if pending and (done + 1) % step == 1 % step and done > 1:
                take_weights()
    while pending:
        take_weights()

    last = n - 1

    @pl.when((me > 0) & (me < n - 1))
    def _():
        for p in range(PIECES):
            arrive(last, p)

    for c in range(pn // 2):
        for half in range(2):
            wait_half(c * 2 + (1 - core), half)

    def fetch(shard, half, buf):
        rng = pl.ds(pl.multiple_of(half * half_rows, half_rows), half_rows)

        @pl.when(shard == j)
        def _():
            pltpu.make_async_copy(weights.at[rng], wbuf.at[buf], wf_sem.at[buf]).start()

        @pl.when(shard != j)
        def _():
            pltpu.make_async_copy(wall.at[shard, rng], wbuf.at[buf], wf_sem.at[buf]).start()

    def fetched(buf):
        pltpu.make_async_copy(weights.at[pl.ds(0, half_rows)], wbuf.at[buf], wf_sem.at[buf]).wait()

    tile = 256 if half_rows % 256 == 0 else 128

    def multiply(slot, q, half, buf, first_row, size):
        rng = pl.ds(first_row, size)
        cols = pl.ds(pl.multiple_of(q * width, width), width)

        def one(t, carry):
            at_ = pl.ds(pl.multiple_of(t * tile, tile), tile)
            acc[half, rng, at_] += lax.dot_general(
                xn[slot, rng, cols], wbuf[buf, at_, :],
                (((1,), (1,)), ((), ())), preferred_element_type=F32,
            )
            return carry

        lax.fori_loop(0, half_rows // tile, one, 0)

    def item_of(it):
        slot = slot_of(it // (per * 2))
        q = (it // 2) % per
        return slot, q, it % 2

    whole = (n - 1) * per * 2

    slot0, q0, half0 = item_of(0)
    fetch(slot0 * per + q0, half0, 0)

    def full(it, carry):
        buf = it % 2
        slot, q, half = item_of(it)
        slot2, q2, half2 = item_of(it + 1)
        fetch(slot2 * per + q2, half2, 1 - buf)
        fetched(buf)
        multiply(slot, q, half, buf, 0, count)
        return carry

    lax.fori_loop(0, whole, full, 0)

    def stage_copy(p):
        return pltpu.make_async_copy(
            stage, qkv.at[:, pl.ds(pl.multiple_of(p * pr, pr), pr), :], out_sem
        )

    heads_half = half_rows // DH
    items = PIECES * per * 2
    slot_last = slot_of(last)

    def tail(it, carry):
        p = it // (per * 2)
        q, half = (it // 2) % per, it % 2
        buf = (whole + it) % 2

        @pl.when(it + 1 < items)
        def _():
            nxt = it + 1
            fetch(slot_last * per + (nxt // 2) % per, nxt % 2, 1 - buf)

        @pl.when(it % (per * 2) == 0)
        def _():
            @pl.when((me == 0) | (me == n - 1))
            def _():
                arrive(last, p)

            normalise(slot_last, p)

        fetched(buf)
        multiply(slot_last, q, half, buf, pl.multiple_of(p * pr, pr), pr)

        @pl.when(it % (per * 2) == per * 2 - 1)
        def _():
            @pl.when(p > 0)
            def _():
                stage_copy(p - 1).wait()

            rng = pl.ds(pl.multiple_of(p * pr, pr), pr)
            cos, sin = ctab[rng, :], stab[rng, :]
            for head in range(groups * HEADS):
                off = head % heads_half * DH
                u = acc[head // heads_half, rng, off : off + DH]
                if head % HEADS < GROUP + 1:
                    u = u * cos + pltpu.roll(u, DH // 2, 1) * sin
                to = head % HEADS * DH
                stage[head // HEADS, :, to : to + DH] = u.astype(BF16)
            stage_copy(p).start()

        return carry

    lax.fori_loop(0, items, tail, 0)
    stage_copy(PIECES - 1).wait()

    for copy in started:
        copy.wait_send()
    for d in range(1, n):
        meta_copy(d).wait_send()

    def drain(i, carry):
        slot, p = i // PIECES, i % PIECES

        @pl.when((slot >= me) & (me > 0))
        def _():
            piece(slot, p, False).wait_send()

        @pl.when((slot <= me) & (me < n - 1))
        def _():
            piece(slot, p, True).wait_send()

        return carry

    lax.fori_loop(0, n * PIECES, drain, 0)


def project(n, pn, groups, tokens, gain, seg, weights):
    count, local = tokens.shape
    rows, width = weights.shape
    half_rows = rows // 2
    metas = (count + local) // LANES
    dma = pltpu.SemaphoreType.DMA
    flops = 2 * count * local * n * rows
    return pl.pallas_call(
        functools.partial(project_kernel, n, pn),
        out_shape=(
            jax.ShapeDtypeStruct((pn, rows, width), BF16),
            jax.ShapeDtypeStruct((groups, count, HEADS * DH), BF16),
        ),
        in_specs=[
            pl.BlockSpec(memory_space=pl.ANY),
            pl.BlockSpec(memory_space=pltpu.VMEM),
            pl.BlockSpec(memory_space=pltpu.VMEM),
            pl.BlockSpec(memory_space=pl.ANY),
        ],
        out_specs=(pl.BlockSpec(memory_space=pl.ANY), pl.BlockSpec(memory_space=pl.ANY)),
        scratch_shapes=[
            pltpu.VMEM((n, count, local), BF16),
            pltpu.VMEM((n, count, local), BF16),
            pltpu.VMEM((2, count, half_rows), F32),
            pltpu.VMEM((2, half_rows, width), BF16),
            pltpu.VMEM((n, metas, LANES), F32),
            pltpu.VMEM((count, LANES), F32),
            pltpu.VMEM((count, LANES), F32),
            pltpu.VMEM((count, LANES), F32),
            pltpu.VMEM((groups, count // PIECES, HEADS * DH), BF16),
            dma,
            dma((2, n, PIECES)),
            dma((n, PIECES)),
            dma((n,)),
            dma((n,)),
            dma((3, pn, 2)),
            dma((pn, 2)),
            dma((2,)),
            dma,
        ],
        compiler_params=pltpu.CompilerParams(
            collective_id=0, has_side_effects=True, vmem_limit_bytes=60 << 20
        ),
        cost_estimate=pl.CostEstimate(flops=flops, bytes_accessed=60 << 20, transcendentals=0),
        name="project",
    )(tokens, gain, seg, weights)


def attend_kernel(
    pn, window, q_ref, k_ref, v_ref, seg, wall, weights, out, rows_out, buf, in_sem, out_sem
):
    g, c = pl.program_id(0), pl.program_id(1)
    steps = pl.num_programs(0) * pl.num_programs(1)
    step = g * pl.num_programs(1) + c
    j = lax.axis_index("pp")
    groups, kept, full = rows_out.shape
    width = full // pn
    row_size = weights.shape[0] // groups

    def pull(gg, s):
        rng = pl.ds(gg * row_size + j * kept, kept)

        @pl.when(s == j)
        def _():
            pltpu.make_async_copy(weights.at[rng], buf.at[gg, s], in_sem.at[gg, s]).start()

        @pl.when(s != j)
        def _():
            pltpu.make_async_copy(wall.at[s, rng], buf.at[gg, s], in_sem.at[gg, s]).start()

    def push(gg, s):
        return pltpu.make_async_copy(
            buf.at[gg, s], rows_out.at[gg, :, pl.ds(s * width, width)], out_sem.at[gg, s]
        )

    @pl.when(step == 0)
    def _():
        for gg in range(groups):
            for s in range(pn):
                pull(gg, s)

    @pl.when(step == 1)
    def _():
        for gg in range(groups):
            for s in range(pn):
                pltpu.make_async_copy(weights.at[pl.ds(0, kept)], buf.at[gg, s], in_sem.at[gg, s]).wait()
                push(gg, s).start()

    back = window - LANES
    base = pl.multiple_of(jnp.maximum(c * LANES - back, 0), LANES)
    rng = pl.ds(base, window)
    own = jnp.broadcast_to(
        seg[:, pl.ds(pl.multiple_of(c * LANES, LANES), LANES)].astype(F32), (LANES, LANES)
    ).T[:, 0:1]
    t = lax.broadcasted_iota(jnp.int32, (LANES, window), 0) + c * LANES
    s = lax.broadcasted_iota(jnp.int32, (LANES, window), 1) + base
    bias = jnp.where((seg[:, rng].astype(F32) == own) & (s <= t), 0.0, -1e30)
    keys = k_ref[0, rng, :]
    values = jnp.concatenate([v_ref[0, rng, :], jnp.ones((window, DH), BF16)], axis=1)
    scale = math.log2(math.e) / math.sqrt(DH)
    for h in range(GROUP):
        cols = slice(h * DH, (h + 1) * DH)
        score = lax.dot_general(
            q_ref[0, :, cols], keys, (((1,), (1,)), ((), ())), preferred_element_type=F32
        )
        score = score * scale + bias
        top = jnp.max(score, axis=1, keepdims=True)
        prob = jnp.exp2(score - top).astype(BF16)
        both = jnp.dot(prob, values, preferred_element_type=F32)
        out[:, cols] = (both[:, :DH] / both[:, DH:]).astype(BF16)

    @pl.when(step == steps - 1)
    def _():
        for gg in range(groups):
            for ss in range(pn):
                push(gg, ss).wait()


def attend(pn, qkv, seg, wall, weights):
    groups, count, _ = qkv.shape
    kept = weights.shape[0] // groups // pn
    width = weights.shape[1]
    window = min(count, MAX_SEQUENCE + LANES)
    dma = pltpu.SemaphoreType.DMA
    return pl.pallas_call(
        functools.partial(attend_kernel, pn, window),
        grid=(groups, count // LANES),
        in_specs=[
            pl.BlockSpec((1, LANES, GROUP * DH), lambda g, c: (g, c, 0)),
            pl.BlockSpec((1, count, DH), lambda g, c: (g, 0, GROUP)),
            pl.BlockSpec((1, count, DH), lambda g, c: (g, 0, GROUP + 1)),
            pl.BlockSpec(memory_space=pltpu.VMEM),
            pl.BlockSpec(memory_space=pl.ANY),
            pl.BlockSpec(memory_space=pl.ANY),
        ],
        out_specs=(
            pl.BlockSpec((LANES, GROUP * DH), lambda g, c: (c, g)),
            pl.BlockSpec(memory_space=pl.ANY),
        ),
        out_shape=(
            jax.ShapeDtypeStruct((count, groups * GROUP * DH), BF16),
            jax.ShapeDtypeStruct((groups, kept, pn * width), BF16),
        ),
        scratch_shapes=[
            pltpu.VMEM((groups, pn, kept, width), BF16),
            dma((groups, pn)),
            dma((groups, pn)),
        ],
        compiler_params=pltpu.CompilerParams(
            dimension_semantics=("arbitrary", "arbitrary"), vmem_limit_bytes=48 << 20
        ),
        name="attend",
    )(qkv, qkv, qkv, seg, wall, weights)


def layer(n, pn, tokens, norm_gain, weights_gen, segment_ids):
    groups, rows, width = weights_gen.shape
    weights = weights_gen.reshape(groups * rows, width)
    gain = norm_gain.astype(F32).reshape(-1, LANES)
    wall, qkv = project(n, pn, groups, tokens, gain, segment_ids, weights)
    attended, weights_rows = attend(pn, qkv, segment_ids, wall, weights)
    return (weights_rows, attended)


def solution(mesh):
    in_specs = (P("pp", "tp"), P("tp"), P("tp", None, "pp"), P("pp", None))
    out_specs = (P("tp", "pp", None), P("pp", "tp"))
    return jax.shard_map(
        functools.partial(layer, mesh.shape["tp"], mesh.shape["pp"]),
        mesh=mesh,
        in_specs=in_specs,
        out_specs=out_specs,
        check_vma=False,
    )
```

```python
import functools
import math

import jax
import jax.numpy as jnp
from jax import lax
from jax.experimental import pallas as pl
from jax.experimental.pallas import tpu as pltpu
from jax.sharding import PartitionSpec as P

DH = 128
GROUP = 8
HEADS = GROUP + 2
LANES = 128
MAX_SEQUENCE = 512
ROPE_BASE = 500000.0
EPS = 1e-05
UNITS = 4
MESH = pl.DeviceIdType.MESH
F32 = jnp.float32
BF16 = jnp.bfloat16


def attend_rows(c, base, window, seg, load_q, keys, values, store):
    mine = pl.ds(pl.multiple_of(c * LANES, LANES), LANES)
    own = jnp.broadcast_to(seg[:, mine].astype(F32), (LANES, LANES)).T[:, 0:1]
    t = lax.broadcasted_iota(jnp.int32, (LANES, window), 0) + c * LANES
    s = lax.broadcasted_iota(jnp.int32, (LANES, window), 1) + base
    bias = jnp.where((seg[:, pl.ds(base, window)].astype(F32) == own) & (s <= t), 0.0, -1e30)
    values = jnp.concatenate([values, jnp.ones((window, DH), BF16)], axis=1)
    scale = math.log2(math.e) / math.sqrt(DH)
    for h in range(GROUP):
        cols = slice(h * DH, (h + 1) * DH)
        score = lax.dot_general(
            load_q(cols), keys, (((1,), (1,)), ((), ())), preferred_element_type=F32
        )
        score = score * scale + bias
        top = jnp.max(score, axis=1, keepdims=True)
        prob = jnp.exp2(score - top).astype(BF16)
        both = jnp.dot(prob, values, preferred_element_type=F32)
        store(cols, (both[:, :DH] / both[:, DH:]).astype(BF16))


def project_kernel(
    n, pn, tokens, gain_in, seg_in, weights,
    wall, query, kv_out, att,
    xr, xn, acc, wbuf, meta, rsb, ctab, stab, stage, kv, astage, gain, seg,
    own_sem, zs_sem, zr_sem, ms_sem, mr_sem, ws_sem, wr_sem, wf_sem, out_sem,
):
    me = lax.axis_index("tp")
    j = lax.axis_index("pp")
    count, local = tokens.shape
    rows, width = weights.shape
    half_rows = rows // 2
    per = local // width
    groups = query.shape[0]
    window = min(count, MAX_SEQUENCE + LANES)
    pr = count // UNITS
    big = count // 2
    rings = pn // 4
    blocks = count // LANES
    core, x, y = j % 2, (j // 2) % 2, j // 4

    def at(y_, x_, core_):
        return (y_ * 2 + x_) * 2 + core_

    j_x = at(y, 1 - x, core)
    j_next = at((y + 1) % rings, x, core)
    j_prev = at((y + rings - 1) % rings, x, core)
    j_pair = at(y, x, 1 - core)

    barrier = pltpu.get_barrier_semaphore()
    for d in range(1, n):
        pl.semaphore_signal(barrier, inc=1, device_id={"tp": (me + d) % n}, device_id_type=MESH)
    for other in (j_x, j_next, j_prev, j_pair):
        pl.semaphore_signal(barrier, inc=1, device_id={"pp": other}, device_id_type=MESH)
    pl.semaphore_wait(barrier, n - 1 + 4)

    parts = [(pl.ds(u * pr, pr), slice(None)) for u in range(UNITS - 1)]
    parts += [(pl.ds(count - pr, pr), pl.ds(h * (local // 2), local // 2)) for h in range(2)]

    def piece(slot, p, up, own=False, part=None):
        if part is None:
            index, sem = (pl.ds(pl.multiple_of(p * big, big), big), slice(None)), p
        else:
            index, sem = parts[part], part
        return pltpu.make_async_remote_copy(
            src_ref=tokens.at[index] if own else xr.at[(slot, *index)],
            dst_ref=xr.at[(slot, *index)],
            send_sem=zs_sem.at[1 if up else 0, slot, sem],
            recv_sem=zr_sem.at[slot, sem],
            device_id={"tp": me + 1 if up else me - 1},
            device_id_type=MESH,
        )

    def own_piece(p):
        @pl.when(me < n - 1)
        def _():
            piece(me, p, True, own=True).start()

        @pl.when(me > 0)
        def _():
            piece(me, p, False, own=True).start()

    def pass_on(slot, p, act):
        for up, there, split in (
            (False, (slot > me) & (me > 0), (slot == n - 1) & (me == 1)),
            (True, (slot < me) & (me < n - 1), (slot == 0) & (me == n - 2)),
        ):
            @pl.when(there & jnp.logical_not(split))
            def _():
                act(piece(slot, p, up))

            for half, group in enumerate((range(UNITS // 2), range(UNITS // 2, len(parts)))):
                @pl.when(there & split & (p == half))
                def _():
                    for part in group:
                        act(piece(slot, p, up, part=part))

    started = []

    def send_half(link, shard, half, target, own=False):
        rng = pl.ds(half * half_rows, half_rows)
        copy = pltpu.make_async_remote_copy(
            src_ref=weights.at[rng] if own else wall.at[shard, rng],
            dst_ref=wall.at[shard, rng],
            send_sem=ws_sem.at[link, shard, half],
            recv_sem=wr_sem.at[shard, half],
            device_id={"pp": target},
            device_id_type=MESH,
        )
        copy.start()
        started.append(copy)

    def wait_half(shard, half):
        rng = pl.ds(half * half_rows, half_rows)
        pltpu.make_async_copy(wall.at[shard, rng], wall.at[shard, rng], wr_sem.at[shard, half]).wait()

    own_piece(0)
    send_half(0, j, 0, j_x, own=True)
    send_half(1, j, 1, j_next, own=True)
    send_half(0, j, 1, j_x, own=True)
    send_half(1, j, 0, j_next, own=True)
    send_half(2, j, 0, j_pair, own=True)
    send_half(2, j, 1, j_pair, own=True)

    loads = [
        pltpu.make_async_copy(tokens, xr.at[me], own_sem.at[0]),
        pltpu.make_async_copy(gain_in, gain, own_sem.at[1]),
        pltpu.make_async_copy(seg_in, seg, own_sem.at[2]),
    ]
    for load in loads:
        load.start()
    for load in loads:
        load.wait()

    def squares(a, carry):
        v = xr[me, pl.ds(pl.multiple_of(a * LANES, LANES), LANES), :].astype(F32)
        total = jnp.sum(v * v, axis=1, keepdims=True)
        meta[me, pl.ds(a, 1), :] = jnp.broadcast_to(total, (LANES, LANES)).T[0:1, :]
        return carry

    lax.fori_loop(0, blocks, squares, 0)
    for b in range(local // LANES):
        meta[me, blocks + b : blocks + b + 1, :] = (
            gain[b * LANES : (b + 1) * LANES].astype(F32).reshape(1, LANES)
        )

    def meta_copy(d):
        return pltpu.make_async_remote_copy(
            src_ref=meta.at[me],
            dst_ref=meta.at[me],
            send_sem=ms_sem.at[d],
            recv_sem=mr_sem.at[me],
            device_id={"tp": (me + d) % n},
            device_id_type=MESH,
        )

    for d in range(1, n):
        meta_copy(d).start()
    own_piece(1)

    lane = lax.broadcasted_iota(jnp.int32, (LANES, LANES), 1)
    freq = jnp.exp((lane % (DH // 2)).astype(F32) * (-2.0 * math.log(ROPE_BASE) / DH))
    sign = jnp.where(lane < DH // 2, -1.0, 1.0)
    ids = seg[...].astype(F32)

    def tables(a, carry):
        rng = pl.ds(pl.multiple_of(a * LANES, LANES), LANES)
        own = jnp.broadcast_to(seg[:, rng].astype(F32), (LANES, LANES)).T[:, 0:1]
        first = jnp.sum(jnp.where(ids < own, 1.0, 0.0), axis=1, keepdims=True)
        order = (lax.broadcasted_iota(jnp.int32, (LANES, LANES), 0) + a * LANES).astype(F32)
        angle = (order - first) * freq
        ctab[rng, :] = jnp.cos(angle)
        stab[rng, :] = jnp.sin(angle) * sign
        return carry

    lax.fori_loop(0, blocks, tables, 0)

    def clear(a, carry):
        rng = pl.ds(pl.multiple_of(a * LANES, LANES), LANES)
        for half in range(2):
            acc[half, rng, :] = jnp.zeros((LANES, half_rows), F32)
        for g in range(groups):
            kv[g, rng, :] = jnp.zeros((LANES, 2 * DH), BF16)
        return carry

    lax.fori_loop(0, blocks, clear, 0)

    for d in range(1, n):
        other = (me + d) % n
        pltpu.make_async_copy(meta.at[other], meta.at[other], mr_sem.at[other]).wait()

    def scales(a, carry):
        total = meta[0, pl.ds(a, 1), :]
        for s in range(1, n):
            total = total + meta[s, pl.ds(a, 1), :]
        scale = lax.rsqrt(total * (1.0 / (n * local)) + EPS)
        rsb[pl.ds(pl.multiple_of(a * LANES, LANES), LANES), :] = jnp.broadcast_to(scale, (LANES, LANES)).T
        return carry

    lax.fori_loop(0, blocks, scales, 0)

    def normalise(slot, p, lanes=(0, local // LANES)):
        def block(a, carry):
            rng = pl.ds(pl.multiple_of(p * pr + a * LANES, LANES), LANES)
            scale = rsb[rng, :]
            for b in range(*lanes):
                cols = slice(b * LANES, (b + 1) * LANES)
                v = xr[slot, rng, cols].astype(F32) * scale
                xn[slot, rng, cols] = (v * meta[slot, blocks + b : blocks + b + 1, :]).astype(BF16)
            return carry

        lax.fori_loop(0, pr // LANES, block, 0)

    near = jnp.minimum(me, n - 1 - me)

    def slot_of(o):
        pair = jnp.where(o % 2 == 1, me + (o + 1) // 2, me - (o + 1) // 2)
        return jnp.where(o <= 2 * near, pair, jnp.where(me <= n - 1 - me, o, n - 1 - o))

    def arrive(slot, p):
        rng = pl.ds(pl.multiple_of(p * big, big), big)
        pltpu.make_async_copy(xr.at[slot, rng], xr.at[slot, rng], zr_sem.at[slot, p]).wait()
        pass_on(slot, p, lambda copy: copy.start())

    def each_piece(p, carry):
        normalise(me, p)
        return carry

    lax.fori_loop(0, UNITS, each_piece, 0)

    def events():
        result = []
        for s in range(1, rings):
            y_s = (y + rings - s) % rings
            on = s < rings - 1
            mine, across = at(y_s, x, core), at(y_s, 1 - x, core)
            result.append([(mine, 1, [(0, j_x)] + ([(1, j_next)] if on else []))])
            if s == 1:
                result[-1].append((j_x, 0, [(1, j_next)]))
            result.append([(mine, 0, [(1, j_next)] if on else [])])
            if s == 1:
                result[-1].append((j_x, 1, []))
            result.append([(across, 0, [(1, j_next)] if on else []), (across, 1, [])])
        return result

    pending = events()

    def take_weights():
        for shard, half, links in pending.pop(0):
            wait_half(shard, half)
            for link, target in links:
                send_half(link, shard, half, target)
            send_half(2, shard, half, j_pair)

    def both_ways(u, carry):
        hop, p = u // 2 + 1, u % 2
        above, below = me + hop, me - hop

        @pl.when(above < n)
        def _():
            arrive(above, p)

        @pl.when(below >= 0)
        def _():
            arrive(below, p)

        @pl.when(above < n)
        def _():
            normalise(above, 2 * p)
            normalise(above, 2 * p + 1)

        @pl.when(below >= 0)
        def _():
            normalise(below, 2 * p)
            normalise(below, 2 * p + 1)

        return carry

    def fetch(shard, half, buf):
        rng = pl.ds(pl.multiple_of(half * half_rows, half_rows), half_rows)

        @pl.when(shard == j)
        def _():
            pltpu.make_async_copy(weights.at[rng], wbuf.at[buf], wf_sem.at[buf]).start()

        @pl.when(shard != j)
        def _():
            pltpu.make_async_copy(wall.at[shard, rng], wbuf.at[buf], wf_sem.at[buf]).start()

    def fetched(buf):
        pltpu.make_async_copy(weights.at[pl.ds(0, half_rows)], wbuf.at[buf], wf_sem.at[buf]).wait()

    tile = 256 if half_rows % 256 == 0 else 128

    def multiply(slot, q, half, buf, first_row, size):
        rng = pl.ds(first_row, size)
        cols = pl.ds(pl.multiple_of(q * width, width), width)

        def one(t, carry):
            at_ = pl.ds(pl.multiple_of(t * tile, tile), tile)
            acc[half, rng, at_] += lax.dot_general(
                xn[slot, rng, cols], wbuf[buf, at_, :],
                (((1,), (1,)), ((), ())), preferred_element_type=F32,
            )
            return carry

        lax.fori_loop(0, half_rows // tile, one, 0)

    held = per * 2

    def slot_weights(slot):
        for i in range(held):
            fetch(slot * per + i // 2, i % 2, i)

    def do_slot(slot):
        slot_weights(slot)

        def one(i, carry):
            fetched(i)
            multiply(slot, i // 2, i % 2, i, 0, count)
            return carry

        lax.fori_loop(0, held, one, 0)

    def from_pair(y_, x_):
        for half in range(2):
            wait_half(at(y_, x_, 1 - core), half)

    last = n - 1
    slot_last = slot_of(last)

    stop = (n - 2) * 2
    times = [min(stop, i * half_rows * width // (big * local)) for i in range(1, len(pending) + 1)]
    if n == 4 and rings == 2 and per == 2:
        pairs = [(y, x), (y, 1 - x), (1 - y, x), (1 - y, 1 - x)]
        slots = [y_ * 2 + x_ for y_, x_ in pairs]
        early = [jnp.abs(me - slot) <= 1 for slot in slots[:3]]
        lax.fori_loop(0, 1, both_ways, 0)
        take_weights()
        lax.fori_loop(1, 2, both_ways, 0)
        from_pair(*pairs[0])
        pl.when(early[0])(lambda: do_slot(slots[0]))
        take_weights()
        for r in (1, 2):
            from_pair(*pairs[r])
            pl.when(early[r])(functools.partial(do_slot, slots[r]))
        lax.fori_loop(2, 3, both_ways, 0)
        take_weights()
        lax.fori_loop(3, stop, both_ways, 0)
        from_pair(*pairs[3])
        for r, slot in enumerate(slots):
            late = slot != slot_last
            if r < 3:
                late = late & jnp.logical_not(early[r])
            pl.when(late)(functools.partial(do_slot, slot))
    else:
        now = 0
        for until in times:
            lax.fori_loop(now, until, both_ways, 0)
            now = until
            take_weights()
        lax.fori_loop(now, stop, both_ways, 0)
        for c in range(pn // 2):
            for half in range(2):
                wait_half(c * 2 + (1 - core), half)

        def in_order(o, carry):
            do_slot(slot_of(o))
            return carry

        lax.fori_loop(0, last, in_order, 0)

    slot_weights(slot_last)
    for i in range(held):
        fetched(i)

    heads_half = half_rows // DH
    items = UNITS * held
    subs = pr // LANES

    def kv_copy(p):
        rng = pl.ds(pl.multiple_of(p * pr, pr), pr)
        return pltpu.make_async_copy(kv.at[:, rng, :], kv_out.at[:, rng, :], out_sem.at[0])

    def att_copy(p):
        return pltpu.make_async_copy(
            astage, att.at[:, pl.ds(pl.multiple_of(p * pr, pr), pr), :], out_sem.at[1]
        )

    query_copy = pltpu.make_async_copy(stage, query, out_sem.at[1])

    def rotate(p):
        rng = pl.ds(pl.multiple_of(p * pr, pr), pr)
        cos, sin = ctab[rng, :], stab[rng, :]
        for head in range(groups * HEADS):
            off = head % heads_half * DH
            u = acc[head // heads_half, rng, off : off + DH]
            g, h = head // HEADS, head % HEADS
            if h < GROUP + 1:
                u = u * cos + pltpu.roll(u, DH // 2, 1) * sin
            if h < GROUP:
                stage[g, :, h * DH : (h + 1) * DH] = u.astype(BF16)
            else:
                kv[g, rng, (h - GROUP) * DH : (h - GROUP + 1) * DH] = u.astype(BF16)

    def attention(p):
        def one(i, carry):
            g, sub = i // subs, i % subs
            rows_ = pl.ds(pl.multiple_of(sub * LANES, LANES), LANES)
            c = p * subs + sub
            base = pl.multiple_of(jnp.maximum(c * LANES - (window - LANES), 0), LANES)
            rng = pl.ds(base, window)

            def load_q(cols):
                return stage[g, rows_, cols]

            def store(cols, value):
                astage[g, rows_, cols] = value

            attend_rows(
                c, base, window, seg, load_q, kv[g, rng, :DH], kv[g, rng, DH:], store
            )
            return carry

        lax.fori_loop(0, groups * subs, one, 0)

    def tail(it, carry):
        p, buf = it // held, it % held
        q, half = buf // 2, buf % 2

        end = (me == 0) | (me == n - 1)
        middle = local // LANES // 2

        def take(part):
            view = xr.at[(slot_last, *parts[part])]
            pltpu.make_async_copy(view, view, zr_sem.at[slot_last, part]).wait()

        @pl.when(end & (buf == 0) & (p < UNITS - 1))
        def _():
            for part in range(UNITS - 1):
                pl.when(p == part)(functools.partial(take, part))
            normalise(slot_last, p)

        @pl.when(end & (buf == 0) & (p == UNITS - 1))
        def _():
            take(UNITS - 1)
            normalise(slot_last, UNITS - 1, (0, middle))

        @pl.when(end & (buf == held // 2) & (p == UNITS - 1))
        def _():
            take(UNITS)
            normalise(slot_last, UNITS - 1, (middle, local // LANES))

        multiply(slot_last, q, half, buf, pl.multiple_of(p * pr, pr), pr)

        @pl.when(it % held == held - 1)
        def _():
            rotate(p)

            @pl.when(p > 0)
            def _():
                kv_copy(p - 1).wait()

            kv_copy(p).start()

            @pl.when(p < UNITS - 1)
            def _():
                @pl.when(p > 0)
                def _():
                    att_copy(p - 1).wait()

                attention(p)
                att_copy(p).start()

        return carry

    lax.fori_loop(0, items, tail, 0)
    att_copy(UNITS - 2).wait()
    query_copy.start()
    kv_copy(UNITS - 1).wait()
    query_copy.wait()

    for copy in started:
        copy.wait_send()
    for d in range(1, n):
        meta_copy(d).wait_send()

    def drain(slot, carry):
        for p in range(2):
            @pl.when(slot != me)
            def _():
                pass_on(slot, p, lambda copy: copy.wait_send())

            @pl.when((slot == me) & (me < n - 1))
            def _():
                piece(me, p, True).wait_send()

            @pl.when((slot == me) & (me > 0))
            def _():
                piece(me, p, False).wait_send()

        return carry

    lax.fori_loop(0, n, drain, 0)


def project(n, pn, groups, tokens, gain, seg, weights):
    count, local = tokens.shape
    rows, width = weights.shape
    half_rows = rows // 2
    metas = (count + local) // LANES
    pr = count // UNITS
    held = local // width * 2
    dma = pltpu.SemaphoreType.DMA
    flops = 2 * count * local * n * rows
    return pl.pallas_call(
        functools.partial(project_kernel, n, pn),
        out_shape=(
            jax.ShapeDtypeStruct((pn, rows, width), BF16),
            jax.ShapeDtypeStruct((groups, pr, GROUP * DH), BF16),
            jax.ShapeDtypeStruct((groups, count, 2 * DH), BF16),
            jax.ShapeDtypeStruct((groups, count, GROUP * DH), BF16),
        ),
        in_specs=[pl.BlockSpec(memory_space=pl.ANY)] * 4,
        out_specs=(pl.BlockSpec(memory_space=pl.ANY),) * 4,
        scratch_shapes=[
            pltpu.VMEM((n, count, local), BF16),
            pltpu.VMEM((n, count, local), BF16),
            pltpu.VMEM((2, count, half_rows), F32),
            pltpu.VMEM((held, half_rows, width), BF16),
            pltpu.VMEM((n, metas, LANES), F32),
            pltpu.VMEM((count, LANES), F32),
            pltpu.VMEM((count, LANES), F32),
            pltpu.VMEM((count, LANES), F32),
            pltpu.VMEM((groups, pr, GROUP * DH), BF16),
            pltpu.VMEM((groups, count, 2 * DH), BF16),
            pltpu.VMEM((groups, pr, GROUP * DH), BF16),
            pltpu.VMEM((local,), BF16),
            pltpu.VMEM((1, count), jnp.int32),
            dma((3,)),
            dma((2, n, UNITS + 1)),
            dma((n, UNITS + 1)),
            dma((n,)),
            dma((n,)),
            dma((3, pn, 2)),
            dma((pn, 2)),
            dma((held,)),
            dma((2,)),
        ],
        compiler_params=pltpu.CompilerParams(
            collective_id=0, has_side_effects=True, vmem_limit_bytes=62 << 20
        ),
        cost_estimate=pl.CostEstimate(flops=flops, bytes_accessed=60 << 20, transcendentals=0),
        name="project",
    )(tokens, gain, seg, weights)


def finish_kernel(
    pn, window, q_ref, kv_ref, seg, wall, weights, att, out, rows_out, buf, abuf, obuf, in_sem, out_sem, a_sem, o_sem
):
    g, sub = pl.program_id(0), pl.program_id(1)
    subs = pl.num_programs(1)
    step = g * subs + sub
    j = lax.axis_index("pp")
    groups, kept, full = rows_out.shape
    width = full // pn
    row_size = weights.shape[0] // groups
    count = att.shape[1]
    before = abuf.shape[1]

    def pull(gg, s):
        rng = pl.ds(gg * row_size + j * kept, kept)

        @pl.when(s == j)
        def _():
            pltpu.make_async_copy(weights.at[rng], buf.at[gg, s], in_sem.at[gg, s]).start()

        @pl.when(s != j)
        def _():
            pltpu.make_async_copy(wall.at[s, rng], buf.at[gg, s], in_sem.at[gg, s]).start()

    def push(gg, s):
        return pltpu.make_async_copy(
            buf.at[gg, s], rows_out.at[gg, :, pl.ds(s * width, width)], out_sem.at[gg, s]
        )

    def pull_rows(gg):
        return pltpu.make_async_copy(att.at[gg, pl.ds(0, before)], abuf.at[gg], a_sem.at[0, gg])

    def push_rows(gg):
        return pltpu.make_async_copy(
            abuf.at[gg], out.at[pl.ds(0, before), pl.ds(gg * GROUP * DH, GROUP * DH)], a_sem.at[1, gg]
        )

    @pl.when(step == 0)
    def _():
        for gg in range(groups):
            pull_rows(gg).start()
            for s in range(pn):
                pull(gg, s)

    c = before // LANES + sub
    base = pl.multiple_of(jnp.maximum(c * LANES - (window - LANES), 0), LANES)
    rng = pl.ds(base, window)

    def load_q(cols):
        return q_ref[0, :, cols]

    def store(cols, value):
        obuf[g, sub, :, cols] = value

    attend_rows(c, base, window, seg, load_q, kv_ref[0, rng, :DH], kv_ref[0, rng, DH:], store)

    def put(gg, ss):
        return pltpu.make_async_copy(
            obuf.at[gg, ss],
            out.at[
                pl.ds(pl.multiple_of(before + ss * LANES, LANES), LANES),
                pl.ds(pl.multiple_of(gg * (GROUP * DH), GROUP * DH), GROUP * DH),
            ],
            o_sem.at[gg, ss],
        )

    put(g, sub).start()

    @pl.when(step == 0)
    def _():
        for gg in range(groups):
            pull_rows(gg).wait()
            push_rows(gg).start()
            for s in range(pn):
                pltpu.make_async_copy(weights.at[pl.ds(0, kept)], buf.at[gg, s], in_sem.at[gg, s]).wait()
                push(gg, s).start()

    @pl.when(step == groups * subs - 1)
    def _():
        for gg in range(groups):
            push_rows(gg).wait()
            for s in range(pn):
                push(gg, s).wait()
            for ss in range(obuf.shape[1]):
                put(gg, ss).wait()


def finish(pn, query, kv, att, seg, wall, weights):
    groups, count, _ = kv.shape
    pr = query.shape[1]
    subs = pr // LANES
    kept = weights.shape[0] // groups // pn
    width = weights.shape[1]
    window = min(count, MAX_SEQUENCE + LANES)
    dma = pltpu.SemaphoreType.DMA
    hold = pl.BlockSpec(memory_space=pl.ANY)
    return pl.pallas_call(
        functools.partial(finish_kernel, pn, window),
        grid=(groups, subs),
        in_specs=[
            pl.BlockSpec((1, LANES, GROUP * DH), lambda g, c: (g, c, 0)),
            pl.BlockSpec((1, count, 2 * DH), lambda g, c: (g, 0, 0)),
            pl.BlockSpec(memory_space=pltpu.VMEM),
            hold,
            hold,
            hold,
        ],
        out_specs=(hold, hold),
        out_shape=(
            jax.ShapeDtypeStruct((count, groups * GROUP * DH), BF16),
            jax.ShapeDtypeStruct((groups, kept, pn * width), BF16),
        ),
        scratch_shapes=[
            pltpu.VMEM((groups, pn, kept, width), BF16),
            pltpu.VMEM((groups, count - pr, GROUP * DH), BF16),
            pltpu.VMEM((groups, subs, LANES, GROUP * DH), BF16),
            dma((groups, pn)),
            dma((groups, pn)),
            dma((2, groups)),
            dma((groups, subs)),
        ],
        compiler_params=pltpu.CompilerParams(
            dimension_semantics=("arbitrary", "arbitrary"), vmem_limit_bytes=63 << 20
        ),
        name="finish",
    )(query, kv, seg, wall, weights, att)


def layer(n, pn, tokens, norm_gain, weights_gen, segment_ids):
    groups, rows, width = weights_gen.shape
    weights = weights_gen.reshape(groups * rows, width)
    wall, query, kv, att = project(n, pn, groups, tokens, norm_gain, segment_ids, weights)
    attended, weights_rows = finish(pn, query, kv, att, segment_ids, wall, weights)
    return (weights_rows, attended)


def solution(mesh):
    in_specs = (P("pp", "tp"), P("tp"), P("tp", None, "pp"), P("pp", None))
    out_specs = (P("tp", "pp", None), P("pp", "tp"))
    return jax.shard_map(
        functools.partial(layer, mesh.shape["tp"], mesh.shape["pp"]),
        mesh=mesh,
        in_specs=in_specs,
        out_specs=out_specs,
        check_vma=False,
    )
```

```python
import functools
import math

import jax
import jax.numpy as jnp
from jax import lax
from jax.experimental import pallas as pl
from jax.experimental.pallas import tpu as pltpu
from jax.sharding import PartitionSpec as P

DH = 128
GROUP = 8
HEADS = GROUP + 2
LANES = 128
MAX_SEQUENCE = 512
ROPE_BASE = 500000.0
EPS = 1e-05
UNITS = 4
MESH = pl.DeviceIdType.MESH
F32 = jnp.float32
BF16 = jnp.bfloat16


def attend_rows(c, base, window, seg, load_q, keys, values, store):
    mine = pl.ds(pl.multiple_of(c * LANES, LANES), LANES)
    own = jnp.broadcast_to(seg[:, mine].astype(F32), (LANES, LANES)).T[:, 0:1]
    t = lax.broadcasted_iota(jnp.int32, (LANES, window), 0) + c * LANES
    s = lax.broadcasted_iota(jnp.int32, (LANES, window), 1) + base
    bias = jnp.where((seg[:, pl.ds(base, window)].astype(F32) == own) & (s <= t), 0.0, -1e30)
    values = jnp.concatenate([values, jnp.ones((window, DH), BF16)], axis=1)
    scale = math.log2(math.e) / math.sqrt(DH)
    for h in range(GROUP):
        cols = slice(h * DH, (h + 1) * DH)
        score = lax.dot_general(
            load_q(cols), keys, (((1,), (1,)), ((), ())), preferred_element_type=F32
        )
        score = score * scale + bias
        top = jnp.max(score, axis=1, keepdims=True)
        prob = jnp.exp2(score - top).astype(BF16)
        both = jnp.dot(prob, values, preferred_element_type=F32)
        store(cols, (both[:, :DH] / both[:, DH:]).astype(BF16))


def project_kernel(
    n, pn, tokens, gain_in, seg_in, weights,
    wall, query, kv_out, att,
    xr, xn, acc, wbuf, meta, rsb, ctab, stab, stage, kv, astage, gain, seg,
    own_sem, zs_sem, zr_sem, ms_sem, mr_sem, ws_sem, wr_sem, wf_sem, out_sem,
):
    me = lax.axis_index("tp")
    j = lax.axis_index("pp")
    count, local = tokens.shape
    rows, width = weights.shape
    half_rows = rows // 2
    per = local // width
    groups = query.shape[0]
    window = min(count, MAX_SEQUENCE + LANES)
    pr = count // UNITS
    big = count // 2
    rings = pn // 4
    blocks = count // LANES
    core, x, y = j % 2, (j // 2) % 2, j // 4

    def at(y_, x_, core_):
        return (y_ * 2 + x_) * 2 + core_

    j_x = at(y, 1 - x, core)
    j_next = at((y + 1) % rings, x, core)
    j_prev = at((y + rings - 1) % rings, x, core)
    j_pair = at(y, x, 1 - core)

    barrier = pltpu.get_barrier_semaphore()
    for d in range(1, n):
        pl.semaphore_signal(barrier, inc=1, device_id={"tp": (me + d) % n}, device_id_type=MESH)
    for other in (j_x, j_next, j_prev, j_pair):
        pl.semaphore_signal(barrier, inc=1, device_id={"pp": other}, device_id_type=MESH)
    pl.semaphore_wait(barrier, n - 1 + 4)

    parts = [(pl.ds(u * pr, pr), slice(None)) for u in range(UNITS - 1)]
    parts += [(pl.ds(count - pr, pr), pl.ds(h * (local // 2), local // 2)) for h in range(2)]

    def piece(slot, p, up, own=False, part=None):
        if part is None:
            index, sem = (pl.ds(pl.multiple_of(p * big, big), big), slice(None)), p
        else:
            index, sem = parts[part], part
        return pltpu.make_async_remote_copy(
            src_ref=tokens.at[index] if own else xr.at[(slot, *index)],
            dst_ref=xr.at[(slot, *index)],
            send_sem=zs_sem.at[1 if up else 0, slot, sem],
            recv_sem=zr_sem.at[slot, sem],
            device_id={"tp": me + 1 if up else me - 1},
            device_id_type=MESH,
        )

    def own_piece(p):
        @pl.when(me < n - 1)
        def _():
            piece(me, p, True, own=True).start()

        @pl.when(me > 0)
        def _():
            piece(me, p, False, own=True).start()

    def pass_on(slot, p, act):
        for up, there, split in (
            (False, (slot > me) & (me > 0), (slot == n - 1) & (me == 1)),
            (True, (slot < me) & (me < n - 1), (slot == 0) & (me == n - 2)),
        ):
            @pl.when(there & jnp.logical_not(split))
            def _():
                act(piece(slot, p, up))

            for half, group in enumerate((range(UNITS // 2), range(UNITS // 2, len(parts)))):
                @pl.when(there & split & (p == half))
                def _():
                    for part in group:
                        act(piece(slot, p, up, part=part))

    started = []

    def send_half(link, shard, half, target, own=False):
        rng = pl.ds(half * half_rows, half_rows)
        copy = pltpu.make_async_remote_copy(
            src_ref=weights.at[rng] if own else wall.at[shard, rng],
            dst_ref=wall.at[shard, rng],
            send_sem=ws_sem.at[link, shard, half],
            recv_sem=wr_sem.at[shard, half],
            device_id={"pp": target},
            device_id_type=MESH,
        )
        copy.start()
        started.append(copy)

    def wait_half(shard, half):
        rng = pl.ds(half * half_rows, half_rows)
        pltpu.make_async_copy(wall.at[shard, rng], wall.at[shard, rng], wr_sem.at[shard, half]).wait()

    own_piece(0)
    send_half(0, j, 0, j_x, own=True)
    send_half(1, j, 1, j_next, own=True)
    send_half(0, j, 1, j_x, own=True)
    send_half(1, j, 0, j_next, own=True)
    send_half(2, j, 0, j_pair, own=True)
    send_half(2, j, 1, j_pair, own=True)

    loads = [
        pltpu.make_async_copy(tokens, xr.at[me], own_sem.at[0]),
        pltpu.make_async_copy(gain_in, gain, own_sem.at[1]),
        pltpu.make_async_copy(seg_in, seg, own_sem.at[2]),
    ]
    for load in loads:
        load.start()
    for load in loads:
        load.wait()

    def squares(a, carry):
        v = xr[me, pl.ds(pl.multiple_of(a * LANES, LANES), LANES), :].astype(F32)
        total = jnp.sum(v * v, axis=1, keepdims=True)
        meta[me, pl.ds(a, 1), :] = jnp.broadcast_to(total, (LANES, LANES)).T[0:1, :]
        return carry

    lax.fori_loop(0, blocks, squares, 0)
    for b in range(local // LANES):
        meta[me, blocks + b : blocks + b + 1, :] = (
            gain[b * LANES : (b + 1) * LANES].astype(F32).reshape(1, LANES)
        )

    def meta_copy(d):
        return pltpu.make_async_remote_copy(
            src_ref=meta.at[me],
            dst_ref=meta.at[me],
            send_sem=ms_sem.at[d],
            recv_sem=mr_sem.at[me],
            device_id={"tp": (me + d) % n},
            device_id_type=MESH,
        )

    for d in range(1, n):
        meta_copy(d).start()
    own_piece(1)

    lane = lax.broadcasted_iota(jnp.int32, (LANES, LANES), 1)
    freq = jnp.exp((lane % (DH // 2)).astype(F32) * (-2.0 * math.log(ROPE_BASE) / DH))
    sign = jnp.where(lane < DH // 2, -1.0, 1.0)
    ids = seg[...].astype(F32)

    def tables(a, carry):
        rng = pl.ds(pl.multiple_of(a * LANES, LANES), LANES)
        own = jnp.broadcast_to(seg[:, rng].astype(F32), (LANES, LANES)).T[:, 0:1]
        first = jnp.sum(jnp.where(ids < own, 1.0, 0.0), axis=1, keepdims=True)
        order = (lax.broadcasted_iota(jnp.int32, (LANES, LANES), 0) + a * LANES).astype(F32)
        angle = (order - first) * freq
        ctab[rng, :] = jnp.cos(angle)
        stab[rng, :] = jnp.sin(angle) * sign
        return carry

    lax.fori_loop(0, blocks, tables, 0)

    def clear(a, carry):
        rng = pl.ds(pl.multiple_of(a * LANES, LANES), LANES)
        for half in range(2):
            acc[half, rng, :] = jnp.zeros((LANES, half_rows), F32)
        for g in range(groups):
            kv[g, rng, :] = jnp.zeros((LANES, 2 * DH), BF16)
        return carry

    lax.fori_loop(0, blocks, clear, 0)

    for d in range(1, n):
        other = (me + d) % n
        pltpu.make_async_copy(meta.at[other], meta.at[other], mr_sem.at[other]).wait()

    def scales(a, carry):
        total = meta[0, pl.ds(a, 1), :]
        for s in range(1, n):
            total = total + meta[s, pl.ds(a, 1), :]
        scale = lax.rsqrt(total * (1.0 / (n * local)) + EPS)
        rsb[pl.ds(pl.multiple_of(a * LANES, LANES), LANES), :] = jnp.broadcast_to(scale, (LANES, LANES)).T
        return carry

    lax.fori_loop(0, blocks, scales, 0)

    def normalise(slot, p, lanes=(0, local // LANES)):
        def block(a, carry):
            rng = pl.ds(pl.multiple_of(p * pr + a * LANES, LANES), LANES)
            scale = rsb[rng, :]
            for b in range(*lanes):
                cols = slice(b * LANES, (b + 1) * LANES)
                v = xr[slot, rng, cols].astype(F32) * scale
                xn[slot, rng, cols] = (v * meta[slot, blocks + b : blocks + b + 1, :]).astype(BF16)
            return carry

        lax.fori_loop(0, pr // LANES, block, 0)

    near = jnp.minimum(me, n - 1 - me)

    def slot_of(o):
        pair = jnp.where(o % 2 == 1, me + (o + 1) // 2, me - (o + 1) // 2)
        return jnp.where(o <= 2 * near, pair, jnp.where(me <= n - 1 - me, o, n - 1 - o))

    def arrive(slot, p):
        rng = pl.ds(pl.multiple_of(p * big, big), big)
        pltpu.make_async_copy(xr.at[slot, rng], xr.at[slot, rng], zr_sem.at[slot, p]).wait()
        pass_on(slot, p, lambda copy: copy.start())

    def each_piece(p, carry):
        normalise(me, p)
        return carry

    lax.fori_loop(0, UNITS, each_piece, 0)

    def events():
        result = []
        for s in range(1, rings):
            y_s = (y + rings - s) % rings
            on = s < rings - 1
            mine, across = at(y_s, x, core), at(y_s, 1 - x, core)
            result.append([(mine, 1, [(0, j_x)] + ([(1, j_next)] if on else []))])
            if s == 1:
                result[-1].append((j_x, 0, [(1, j_next)]))
            result.append([(mine, 0, [(1, j_next)] if on else [])])
            if s == 1:
                result[-1].append((j_x, 1, []))
            result.append([(across, 0, [(1, j_next)] if on else []), (across, 1, [])])
        return result

    pending = events()

    def take_weights():
        for shard, half, links in pending.pop(0):
            wait_half(shard, half)
            for link, target in links:
                send_half(link, shard, half, target)
            send_half(2, shard, half, j_pair)

    def both_ways(u, carry):
        hop, p = u // 2 + 1, u % 2
        above, below = me + hop, me - hop

        @pl.when(above < n)
        def _():
            arrive(above, p)

        @pl.when(below >= 0)
        def _():
            arrive(below, p)

        @pl.when(above < n)
        def _():
            normalise(above, 2 * p)
            normalise(above, 2 * p + 1)

        @pl.when(below >= 0)
        def _():
            normalise(below, 2 * p)
            normalise(below, 2 * p + 1)

        return carry

    def fetch(shard, half, buf):
        rng = pl.ds(pl.multiple_of(half * half_rows, half_rows), half_rows)

        @pl.when(shard == j)
        def _():
            pltpu.make_async_copy(weights.at[rng], wbuf.at[buf], wf_sem.at[buf]).start()

        @pl.when(shard != j)
        def _():
            pltpu.make_async_copy(wall.at[shard, rng], wbuf.at[buf], wf_sem.at[buf]).start()

    def fetched(buf):
        pltpu.make_async_copy(weights.at[pl.ds(0, half_rows)], wbuf.at[buf], wf_sem.at[buf]).wait()

    tile = 256 if half_rows % 256 == 0 else 128

    def multiply(slot, q, half, buf, first_row, size):
        rng = pl.ds(first_row, size)
        cols = pl.ds(pl.multiple_of(q * width, width), width)

        def one(t, carry):
            at_ = pl.ds(pl.multiple_of(t * tile, tile), tile)
            acc[half, rng, at_] += lax.dot_general(
                xn[slot, rng, cols], wbuf[buf, at_, :],
                (((1,), (1,)), ((), ())), preferred_element_type=F32,
            )
            return carry

        lax.fori_loop(0, half_rows // tile, one, 0)

    chunk = 640 if half_rows % 640 == 0 else half_rows

    def multiply_few(slot, q, half, buf, first_row, size):
        rng = pl.ds(first_row, size)
        cols = pl.ds(pl.multiple_of(q * width, width), width)
        for t in range(half_rows // chunk):
            out = lax.dot_general(
                wbuf[buf, t * chunk : (t + 1) * chunk, :], xn[slot, rng, cols],
                (((1,), (1,)), ((), ())), preferred_element_type=F32,
            )
            acc[half, rng, t * chunk : (t + 1) * chunk] += out.T

    held = per * 2

    def slot_weights(slot):
        for i in range(held):
            fetch(slot * per + i // 2, i % 2, i)

    def do_slot(slot):
        slot_weights(slot)

        def one(i, carry):
            fetched(i)
            multiply(slot, i // 2, i % 2, i, 0, count)
            return carry

        lax.fori_loop(0, held, one, 0)

    def from_pair(y_, x_):
        for half in range(2):
            wait_half(at(y_, x_, 1 - core), half)

    last = n - 1
    slot_last = slot_of(last)

    stop = (n - 2) * 2
    times = [min(stop, i * half_rows * width // (big * local)) for i in range(1, len(pending) + 1)]
    if n == 4 and rings == 2 and per == 2:
        pairs = [(y, x), (y, 1 - x), (1 - y, x), (1 - y, 1 - x)]
        slots = [y_ * 2 + x_ for y_, x_ in pairs]
        early = [jnp.abs(me - slot) <= 1 for slot in slots[:3]]
        lax.fori_loop(0, 1, both_ways, 0)
        take_weights()
        lax.fori_loop(1, 2, both_ways, 0)
        from_pair(*pairs[0])
        pl.when(early[0])(lambda: do_slot(slots[0]))
        take_weights()
        for r in (1, 2):
            from_pair(*pairs[r])
            pl.when(early[r])(functools.partial(do_slot, slots[r]))
        lax.fori_loop(2, 3, both_ways, 0)
        take_weights()
        lax.fori_loop(3, stop, both_ways, 0)
        from_pair(*pairs[3])
        for r, slot in enumerate(slots):
            late = slot != slot_last
            if r < 3:
                late = late & jnp.logical_not(early[r])
            pl.when(late)(functools.partial(do_slot, slot))
    else:
        now = 0
        for until in times:
            lax.fori_loop(now, until, both_ways, 0)
            now = until
            take_weights()
        lax.fori_loop(now, stop, both_ways, 0)
        for c in range(pn // 2):
            for half in range(2):
                wait_half(c * 2 + (1 - core), half)

        def in_order(o, carry):
            do_slot(slot_of(o))
            return carry

        lax.fori_loop(0, last, in_order, 0)

    slot_weights(slot_last)
    for i in range(held):
        fetched(i)

    heads_half = half_rows // DH
    items = UNITS * held
    subs = pr // LANES

    def kv_copy(p):
        rng = pl.ds(pl.multiple_of(p * pr, pr), pr)
        return pltpu.make_async_copy(kv.at[:, rng, :], kv_out.at[:, rng, :], out_sem.at[0])

    def att_copy(p):
        return pltpu.make_async_copy(
            astage, att.at[:, pl.ds(pl.multiple_of(p * pr, pr), pr), :], out_sem.at[1]
        )

    query_copy = pltpu.make_async_copy(stage, query, out_sem.at[1])

    def rotate(p):
        rng = pl.ds(pl.multiple_of(p * pr, pr), pr)
        cos, sin = ctab[rng, :], stab[rng, :]
        for head in range(groups * HEADS):
            off = head % heads_half * DH
            u = acc[head // heads_half, rng, off : off + DH]
            g, h = head // HEADS, head % HEADS
            if h < GROUP + 1:
                u = u * cos + pltpu.roll(u, DH // 2, 1) * sin
            if h < GROUP:
                stage[g, :, h * DH : (h + 1) * DH] = u.astype(BF16)
            else:
                kv[g, rng, (h - GROUP) * DH : (h - GROUP + 1) * DH] = u.astype(BF16)

    def attention(p):
        def one(i, carry):
            g, sub = i // subs, i % subs
            rows_ = pl.ds(pl.multiple_of(sub * LANES, LANES), LANES)
            c = p * subs + sub
            base = pl.multiple_of(jnp.maximum(c * LANES - (window - LANES), 0), LANES)
            rng = pl.ds(base, window)

            def load_q(cols):
                return stage[g, rows_, cols]

            def store(cols, value):
                astage[g, rows_, cols] = value

            attend_rows(
                c, base, window, seg, load_q, kv[g, rng, :DH], kv[g, rng, DH:], store
            )
            return carry

        lax.fori_loop(0, groups * subs, one, 0)

    def tail(it, carry):
        p, buf = it // held, it % held
        q, half = buf // 2, buf % 2

        end = (me == 0) | (me == n - 1)
        middle = local // LANES // 2

        def take(part):
            view = xr.at[(slot_last, *parts[part])]
            pltpu.make_async_copy(view, view, zr_sem.at[slot_last, part]).wait()

        @pl.when(end & (buf == 0) & (p < UNITS - 1))
        def _():
            for part in range(UNITS - 1):
                pl.when(p == part)(functools.partial(take, part))
            normalise(slot_last, p)

        @pl.when(end & (buf == 0) & (p == UNITS - 1))
        def _():
            take(UNITS - 1)
            normalise(slot_last, UNITS - 1, (0, middle))

        @pl.when(end & (buf == held // 2) & (p == UNITS - 1))
        def _():
            take(UNITS)
            normalise(slot_last, UNITS - 1, (middle, local // LANES))

        multiply_few(slot_last, q, half, buf, pl.multiple_of(p * pr, pr), pr)

        @pl.when(it % held == held - 1)
        def _():
            rotate(p)

            @pl.when(p > 0)
            def _():
                kv_copy(p - 1).wait()

            kv_copy(p).start()

            @pl.when(p < UNITS - 1)
            def _():
                @pl.when(p > 0)
                def _():
                    att_copy(p - 1).wait()

                attention(p)
                att_copy(p).start()

        return carry

    lax.fori_loop(0, items, tail, 0)
    att_copy(UNITS - 2).wait()
    query_copy.start()
    kv_copy(UNITS - 1).wait()
    query_copy.wait()

    for copy in started:
        copy.wait_send()
    for d in range(1, n):
        meta_copy(d).wait_send()

    def drain(slot, carry):
        for p in range(2):
            @pl.when(slot != me)
            def _():
                pass_on(slot, p, lambda copy: copy.wait_send())

            @pl.when((slot == me) & (me < n - 1))
            def _():
                piece(me, p, True).wait_send()

            @pl.when((slot == me) & (me > 0))
            def _():
                piece(me, p, False).wait_send()

        return carry

    lax.fori_loop(0, n, drain, 0)


def project(n, pn, groups, tokens, gain, seg, weights):
    count, local = tokens.shape
    rows, width = weights.shape
    half_rows = rows // 2
    metas = (count + local) // LANES
    pr = count // UNITS
    held = local // width * 2
    dma = pltpu.SemaphoreType.DMA
    flops = 2 * count * local * n * rows
    return pl.pallas_call(
        functools.partial(project_kernel, n, pn),
        out_shape=(
            jax.ShapeDtypeStruct((pn, rows, width), BF16),
            jax.ShapeDtypeStruct((groups, pr, GROUP * DH), BF16),
            jax.ShapeDtypeStruct((groups, count, 2 * DH), BF16),
            jax.ShapeDtypeStruct((groups, count, GROUP * DH), BF16),
        ),
        in_specs=[pl.BlockSpec(memory_space=pl.ANY)] * 4,
        out_specs=(pl.BlockSpec(memory_space=pl.ANY),) * 4,
        scratch_shapes=[
            pltpu.VMEM((n, count, local), BF16),
            pltpu.VMEM((n, count, local), BF16),
            pltpu.VMEM((2, count, half_rows), F32),
            pltpu.VMEM((held, half_rows, width), BF16),
            pltpu.VMEM((n, metas, LANES), F32),
            pltpu.VMEM((count, LANES), F32),
            pltpu.VMEM((count, LANES), F32),
            pltpu.VMEM((count, LANES), F32),
            pltpu.VMEM((groups, pr, GROUP * DH), BF16),
            pltpu.VMEM((groups, count, 2 * DH), BF16),
            pltpu.VMEM((groups, pr, GROUP * DH), BF16),
            pltpu.VMEM((local,), BF16),
            pltpu.VMEM((1, count), jnp.int32),
            dma((3,)),
            dma((2, n, UNITS + 1)),
            dma((n, UNITS + 1)),
            dma((n,)),
            dma((n,)),
            dma((3, pn, 2)),
            dma((pn, 2)),
            dma((held,)),
            dma((2,)),
        ],
        compiler_params=pltpu.CompilerParams(
            collective_id=0, has_side_effects=True, vmem_limit_bytes=62 << 20
        ),
        cost_estimate=pl.CostEstimate(flops=flops, bytes_accessed=60 << 20, transcendentals=0),
        name="project",
    )(tokens, gain, seg, weights)


def finish_kernel(
    pn, window, q_ref, kv_ref, seg, wall, weights, att, out, rows_out, buf, abuf, obuf, in_sem, out_sem, a_sem, o_sem
):
    g, sub = pl.program_id(0), pl.program_id(1)
    subs = pl.num_programs(1)
    step = g * subs + sub
    j = lax.axis_index("pp")
    groups, kept, full = rows_out.shape
    width = full // pn
    row_size = weights.shape[0] // groups
    count = att.shape[1]
    before = abuf.shape[1]

    def pull(gg, s):
        rng = pl.ds(gg * row_size + j * kept, kept)

        @pl.when(s == j)
        def _():
            pltpu.make_async_copy(weights.at[rng], buf.at[gg, s], in_sem.at[gg, s]).start()

        @pl.when(s != j)
        def _():
            pltpu.make_async_copy(wall.at[s, rng], buf.at[gg, s], in_sem.at[gg, s]).start()

    def push(gg, s):
        return pltpu.make_async_copy(
            buf.at[gg, s], rows_out.at[gg, :, pl.ds(s * width, width)], out_sem.at[gg, s]
        )

    def pull_rows(gg):
        return pltpu.make_async_copy(att.at[gg, pl.ds(0, before)], abuf.at[gg], a_sem.at[0, gg])

    def push_rows(gg):
        return pltpu.make_async_copy(
            abuf.at[gg], out.at[pl.ds(0, before), pl.ds(gg * GROUP * DH, GROUP * DH)], a_sem.at[1, gg]
        )

    @pl.when(step == 0)
    def _():
        for gg in range(groups):
            pull_rows(gg).start()
            for s in range(pn):
                pull(gg, s)

    c = before // LANES + sub
    base = pl.multiple_of(jnp.maximum(c * LANES - (window - LANES), 0), LANES)
    rng = pl.ds(base, window)

    def load_q(cols):
        return q_ref[0, :, cols]

    def store(cols, value):
        obuf[g, sub, :, cols] = value

    attend_rows(c, base, window, seg, load_q, kv_ref[0, rng, :DH], kv_ref[0, rng, DH:], store)

    def put(gg, ss):
        return pltpu.make_async_copy(
            obuf.at[gg, ss],
            out.at[
                pl.ds(pl.multiple_of(before + ss * LANES, LANES), LANES),
                pl.ds(pl.multiple_of(gg * (GROUP * DH), GROUP * DH), GROUP * DH),
            ],
            o_sem.at[gg, ss],
        )

    put(g, sub).start()

    @pl.when(step == 0)
    def _():
        for gg in range(groups):
            pull_rows(gg).wait()
            push_rows(gg).start()
            for s in range(pn):
                pltpu.make_async_copy(weights.at[pl.ds(0, kept)], buf.at[gg, s], in_sem.at[gg, s]).wait()
                push(gg, s).start()

    @pl.when(step == groups * subs - 1)
    def _():
        for gg in range(groups):
            push_rows(gg).wait()
            for s in range(pn):
                push(gg, s).wait()
            for ss in range(obuf.shape[1]):
                put(gg, ss).wait()


def finish(pn, query, kv, att, seg, wall, weights):
    groups, count, _ = kv.shape
    pr = query.shape[1]
    subs = pr // LANES
    kept = weights.shape[0] // groups // pn
    width = weights.shape[1]
    window = min(count, MAX_SEQUENCE + LANES)
    dma = pltpu.SemaphoreType.DMA
    hold = pl.BlockSpec(memory_space=pl.ANY)
    return pl.pallas_call(
        functools.partial(finish_kernel, pn, window),
        grid=(groups, subs),
        in_specs=[
            pl.BlockSpec((1, LANES, GROUP * DH), lambda g, c: (g, c, 0)),
            pl.BlockSpec((1, count, 2 * DH), lambda g, c: (g, 0, 0)),
            pl.BlockSpec(memory_space=pltpu.VMEM),
            hold,
            hold,
            hold,
        ],
        out_specs=(hold, hold),
        out_shape=(
            jax.ShapeDtypeStruct((count, groups * GROUP * DH), BF16),
            jax.ShapeDtypeStruct((groups, kept, pn * width), BF16),
        ),
        scratch_shapes=[
            pltpu.VMEM((groups, pn, kept, width), BF16),
            pltpu.VMEM((groups, count - pr, GROUP * DH), BF16),
            pltpu.VMEM((groups, subs, LANES, GROUP * DH), BF16),
            dma((groups, pn)),
            dma((groups, pn)),
            dma((2, groups)),
            dma((groups, subs)),
        ],
        compiler_params=pltpu.CompilerParams(
            dimension_semantics=("arbitrary", "arbitrary"), vmem_limit_bytes=63 << 20
        ),
        name="finish",
    )(query, kv, seg, wall, weights, att)


def layer(n, pn, tokens, norm_gain, weights_gen, segment_ids):
    groups, rows, width = weights_gen.shape
    weights = weights_gen.reshape(groups * rows, width)
    wall, query, kv, att = project(n, pn, groups, tokens, norm_gain, segment_ids, weights)
    attended, weights_rows = finish(pn, query, kv, att, segment_ids, wall, weights)
    return (weights_rows, attended)


def solution(mesh):
    in_specs = (P("pp", "tp"), P("tp"), P("tp", None, "pp"), P("pp", None))
    out_specs = (P("tp", "pp", None), P("pp", "tp"))
    return jax.shard_map(
        functools.partial(layer, mesh.shape["tp"], mesh.shape["pp"]),
        mesh=mesh,
        in_specs=in_specs,
        out_specs=out_specs,
        check_vma=False,
    )
```
